32 devices in a mesh: task: 4 (over y, core), col: 8 (over z, x).
Axes of the slice: x: 2, y: 2, z: 4, core: 2. Of those that a mesh axis runs over, the one named last changes fastest.
Arguments:
- deltas: bfloat16 [4, 4096, 14336], P('task', None, 'col'), may hold values from -36 to 36
- sketch: bfloat16 [4, 14336, 256], P('task', 'col'), may hold values from -0.06 to 0.06, as said below
Outputs:
- merged: bfloat16 [4096, 14336], P('task', 'col')
The draws below stay inside these ranges and needn't reach their ends.
Inputs may be any that keep to these rules, and one draw needn't show every extreme that they name: `sketch`: entries are drawn independently.
All inputs are finite; a program needn't handle non-finite values.
Results may differ from the reference program's by a relative error of at most 0.012.
Values may be sent and summed in bfloat16 or wider, within the bound.
No kernel may reach another device: no remote copies, remote signals or barrier semaphores. Data moves between devices by JAX's collectives and lax.ppermute only.
A program may use at most 192 MiB of HBM per device.

```python
import math
import jax
import jax.numpy as jnp
from jax import lax

D = 4096
F = 14336
K = 256
ITERS = 1
TASKS = 4


def draw_deltas(key, part):
    first, second, third = jax.random.split(jax.random.fold_in(key, 11), 3)
    values = jnp.clip(jax.random.normal(first, (TASKS, D, F), jnp.float32), -6.0, 6.0)
    row_scale = jnp.exp(jax.random.uniform(second, (1, D, 1), jnp.float32, 0.0, math.log(16.0)))
    col_scale = jnp.exp(jax.random.uniform(third, (TASKS, 1, F), jnp.float32, math.log(0.25), math.log(0.75)))
    return (0.5 * values * row_scale * col_scale).astype(jnp.bfloat16)


def draw_sketch(key, part):
    inner = jax.random.fold_in(key, 23)
    values = jnp.clip(jax.random.normal(inner, (TASKS, F, K), jnp.float32), -6.0, 6.0)
    return (values * 0.01).astype(jnp.bfloat16)


def setup_inputs(seed: int = 0) -> dict:
    key_of = jax.random.split(jax.random.key(seed), 3)
    deltas = draw_deltas(jax.random.fold_in(key_of[2], 71), 0)
    sketch = draw_sketch(jax.random.fold_in(key_of[2], 71), 0)
    return dict(deltas=deltas, sketch=sketch)


def orthonormal(product):
    gram = jnp.dot(product.T.astype(jnp.float32), product.astype(jnp.float32), precision=lax.Precision.HIGHEST, preferred_element_type=jnp.float32)
    lower = jnp.linalg.cholesky(gram)
    return jax.scipy.linalg.solve_triangular(lower, product.T, lower=True).T.astype(jnp.bfloat16)

def reference(deltas, sketch):
    bases = []
    coeffs = []
    for task in range(TASKS):
        delta = deltas[task]
        basis = orthonormal(jnp.dot(delta.astype(jnp.float32), sketch[task].astype(jnp.float32), preferred_element_type=jnp.float32))
        for sweep in range(ITERS):
            across = jnp.dot(delta.T.astype(jnp.float32), basis.astype(jnp.float32), preferred_element_type=jnp.float32).astype(jnp.bfloat16)
            basis = orthonormal(jnp.dot(delta.astype(jnp.float32), across.astype(jnp.float32), preferred_element_type=jnp.float32))
        coeffs.append(jnp.dot(basis.T.astype(jnp.float32), delta.astype(jnp.float32), preferred_element_type=jnp.float32).astype(jnp.bfloat16))
        bases.append(basis)
    joined = jnp.concatenate(bases, axis=1)
    stacked = jnp.concatenate(coeffs, axis=0)
    joint = jnp.dot(joined.T.astype(jnp.float32), joined.astype(jnp.float32), preferred_element_type=jnp.float32)
    lower = jnp.linalg.cholesky(joint)
    whitened = jax.scipy.linalg.solve_triangular(lower, joined.astype(jnp.float32).T, lower=True).T.astype(jnp.bfloat16)
    return jnp.dot(whitened.astype(jnp.float32), stacked.astype(jnp.float32), preferred_element_type=jnp.float32).astype(jnp.bfloat16)
```

```python
import jax
import jax.numpy as jnp
from jax import lax
from jax.experimental import pallas as pl
from jax.experimental.pallas import tpu as pltpu
from jax.sharding import PartitionSpec as P

BLOCK = 128
SUB = 8
CHUNK = 256


def dot_exact(lhs, rhs):
    return jnp.dot(lhs, rhs, precision=lax.Precision.HIGHEST, preferred_element_type=jnp.float32)


def inverse_factor_block(block):
    groups = BLOCK // SUB
    rows = lax.broadcasted_iota(jnp.int32, (SUB, BLOCK), 0)
    lanes = lax.broadcasted_iota(jnp.int32, (SUB, BLOCK), 1)
    left = [block[g * SUB : (g + 1) * SUB, :] for g in range(groups)]
    right = [(lanes == rows + g * SUB).astype(jnp.float32) for g in range(groups)]
    for j in range(BLOCK):
        home, sub = divmod(j, SUB)
        column = jnp.broadcast_to(left[home][:, j : j + 1], (SUB, BLOCK))
        inverse = 1.0 / column[sub : sub + 1, :]
        row_left = left[home][sub : sub + 1, :] * inverse
        row_right = right[home][sub : sub + 1, :] * inverse
        for g in range(home, groups):
            if g == home:
                factor = jnp.where(rows > sub, column, 0.0)
            else:
                factor = jnp.broadcast_to(left[g][:, j : j + 1], (SUB, BLOCK))
            left[g] = left[g] - factor * row_left
            right[g] = right[g] - factor * row_right
    scaled = []
    for g in range(groups):
        pivot = jnp.sum(jnp.where(lanes == rows + g * SUB, left[g], 0.0), axis=1, keepdims=True)
        scaled.append(right[g] * lax.rsqrt(pivot))
    return jnp.concatenate(scaled, axis=0)


def eliminate(out_ref, inverse, lo):
    size = out_ref.shape[0]
    hi = lo + BLOCK
    if lo:
        out_ref[lo:hi, :lo] = dot_exact(inverse, out_ref[lo:hi, :lo])
    out_ref[lo:hi, lo:hi] = inverse
    if hi == size:
        return
    panel = dot_exact(inverse, out_ref[lo:hi, hi:])
    out_ref[lo:hi, hi:] = jnp.zeros_like(panel)
    turned = panel.T
    for top in range(hi, size, CHUNK):
        end = min(top + CHUNK, size)
        part = turned[top - hi : end - hi, :]
        out_ref[top:end, top:] -= dot_exact(part, panel[:, top - hi :])
        if lo:
            out_ref[top:end, :lo] -= dot_exact(part, out_ref[lo:hi, :lo])
        out_ref[top:end, lo:hi] = -dot_exact(part, inverse)


def inverse_factor_kernel(gram_ref, out_ref, block_ref):
    steps = gram_ref.shape[0] // BLOCK
    out_ref[...] = gram_ref[...]
    block_ref[...] = gram_ref[:BLOCK, :BLOCK]

    @pl.loop(0, steps)
    def _(step):
        block_ref[...] = inverse_factor_block(block_ref[...])
        for k in range(steps):

            @pl.when(step == k)
            def _():
                eliminate(out_ref, block_ref[...], k * BLOCK)
                if k + 1 < steps:
                    end = (k + 2) * BLOCK
                    block_ref[...] = out_ref[end - BLOCK : end, end - BLOCK : end]


def inverse_factor(gram):
    return pl.pallas_call(
        inverse_factor_kernel,
        out_shape=jax.ShapeDtypeStruct(gram.shape, jnp.float32),
        scratch_shapes=[pltpu.VMEM((BLOCK, BLOCK), jnp.float32)],
        compiler_params=pltpu.CompilerParams(vmem_limit_bytes=48 * 1024 * 1024),
        name="inverse_factor",
    )(gram)


def summed(partial):
    devices = lax.axis_size("col")
    rows = partial.shape[0] // devices
    parts = lax.all_to_all(partial.astype(jnp.bfloat16), "col", 0, 0, tiled=True)
    parts = parts.reshape(devices, rows, partial.shape[1])
    return jnp.sum(parts.astype(jnp.float32), axis=0).astype(jnp.bfloat16)


def product(lhs, rhs, contract):
    return lax.dot_general(lhs, rhs, (contract, ((), ())), preferred_element_type=jnp.float32)


ROWS = ((0,), (0,))
INNER = ((1,), (0,))


def shards(deltas, sketch):
    delta = deltas[0]
    first = lax.all_gather(summed(product(delta, sketch[0], INNER)), "col", axis=0, tiled=True)
    norms = jnp.sum(jnp.square(first.astype(jnp.float32)), axis=0, keepdims=True)
    across = (product(delta, first, ROWS) * lax.rsqrt(norms)).astype(jnp.bfloat16)
    tasks = lax.axis_size("task")
    ranges = lax.all_gather(summed(product(delta, across, INNER)), ("task", "col"), axis=0, tiled=True)
    ranges = ranges.reshape(tasks, delta.shape[0], -1)
    ranged = lax.dynamic_index_in_dim(ranges, lax.axis_index("task"), 0, keepdims=False)
    inverse = inverse_factor(product(ranged, ranged, ROWS))
    coeffs = dot_exact(inverse, product(ranged, delta, ROWS)).astype(jnp.bfloat16)
    stacked = lax.all_gather(coeffs, "task", axis=0, tiled=True)
    joined = jnp.concatenate([ranges[t] for t in range(tasks)], axis=1)
    joint = inverse_factor(product(joined, joined, ROWS))
    row_count = joined.shape[0] // tasks
    joined_rows = lax.dynamic_slice_in_dim(joined, lax.axis_index("task") * row_count, row_count, 0)
    whitened = lax.dot_general(
        joined_rows.astype(jnp.float32),
        joint,
        (((1,), (1,)), ((), ())),
        precision=lax.Precision.HIGHEST,
        preferred_element_type=jnp.float32,
    ).astype(jnp.bfloat16)
    return product(whitened, stacked, INNER).astype(jnp.bfloat16)


def solution(mesh):
    in_specs = (P("task", None, "col"), P("task", "col", None))
    out_specs = P("task", "col")
    return jax.shard_map(shards, mesh=mesh, in_specs=in_specs, out_specs=out_specs, check_vma=False)
```

```python
import jax
import jax.numpy as jnp
from jax import lax
from jax.experimental import pallas as pl
from jax.experimental.pallas import tpu as pltpu
from jax.sharding import PartitionSpec as P

BLOCK = 128
SUB = 8
STRIDE = 4
CHUNK = 256


def dot_exact(lhs, rhs):
    return jnp.dot(lhs, rhs, precision=lax.Precision.HIGHEST, preferred_element_type=jnp.float32)


def inverse_factor_block(block):
    groups = BLOCK // SUB
    rows = lax.broadcasted_iota(jnp.int32, (SUB, BLOCK), 0)
    lanes = lax.broadcasted_iota(jnp.int32, (SUB, BLOCK), 1)
    left = [block[g * SUB : (g + 1) * SUB, :] for g in range(groups)]
    right = [(lanes == rows + g * SUB).astype(jnp.float32) for g in range(groups)]
    for start in range(0, BLOCK, STRIDE):
        home, base = divmod(start, SUB)

        def columns_of(g):
            part = left[g]
            return [jnp.broadcast_to(part[:, j : j + 1], (SUB, BLOCK)) for j in range(start, start + STRIDE)]

        columns = columns_of(home)
        pivots = []
        for k in range(STRIDE):
            sub = base + k
            inverse = 1.0 / columns[k][sub : sub + 1, :]
            row_left = left[home][sub : sub + 1, :] * inverse
            row_right = right[home][sub : sub + 1, :] * inverse
            ahead = [columns[m][sub : sub + 1, :] * inverse for m in range(k + 1, STRIDE)]
            pivots.append((row_left, row_right, ahead))
            factor = jnp.where(rows > sub, columns[k], 0.0)
            left[home] = left[home] - factor * row_left
            right[home] = right[home] - factor * row_right
            for m in range(k + 1, STRIDE):
                columns[m] = columns[m] - factor * ahead[m - k - 1]
        for g in range(home + 1, groups):
            columns = columns_of(g)
            for k, (row_left, row_right, ahead) in enumerate(pivots):
                left[g] = left[g] - columns[k] * row_left
                right[g] = right[g] - columns[k] * row_right
                for m in range(k + 1, STRIDE):
                    columns[m] = columns[m] - columns[k] * ahead[m - k - 1]
    scaled = []
    for g in range(groups):
        pivot = jnp.sum(jnp.where(lanes == rows + g * SUB, left[g], 0.0), axis=1, keepdims=True)
        scaled.append(right[g] * lax.rsqrt(pivot))
    return jnp.concatenate(scaled, axis=0)


def eliminate(out_ref, inverse, lo):
    size = out_ref.shape[0]
    hi = lo + BLOCK
    if lo:
        out_ref[lo:hi, :lo] = dot_exact(inverse, out_ref[lo:hi, :lo])
    out_ref[lo:hi, lo:hi] = inverse
    if hi == size:
        return
    panel = dot_exact(inverse, out_ref[lo:hi, hi:])
    out_ref[lo:hi, hi:] = jnp.zeros_like(panel)
    turned = panel.T
    for top in range(hi, size, CHUNK):
        end = min(top + CHUNK, size)
        part = turned[top - hi : end - hi, :]
        out_ref[top:end, top:] -= dot_exact(part, panel[:, top - hi :])
        if lo:
            out_ref[top:end, :lo] -= dot_exact(part, out_ref[lo:hi, :lo])
        out_ref[top:end, lo:hi] = -dot_exact(part, inverse)


def inverse_factor_kernel(gram_ref, out_ref, block_ref):
    steps = gram_ref.shape[0] // BLOCK
    out_ref[...] = gram_ref[...]
    block_ref[...] = gram_ref[:BLOCK, :BLOCK]

    @pl.loop(0, steps)
    def _(step):
        block_ref[...] = inverse_factor_block(block_ref[...])
        for k in range(steps):

            @pl.when(step == k)
            def _():
                eliminate(out_ref, block_ref[...], k * BLOCK)
                if k + 1 < steps:
                    end = (k + 2) * BLOCK
                    block_ref[...] = out_ref[end - BLOCK : end, end - BLOCK : end]


def inverse_factor(gram):
    return pl.pallas_call(
        inverse_factor_kernel,
        out_shape=jax.ShapeDtypeStruct(gram.shape, jnp.float32),
        scratch_shapes=[pltpu.VMEM((BLOCK, BLOCK), jnp.float32)],
        compiler_params=pltpu.CompilerParams(vmem_limit_bytes=48 * 1024 * 1024),
        name="inverse_factor",
    )(gram)


def summed(partial):
    devices = lax.axis_size("col")
    rows = partial.shape[0] // devices
    parts = lax.all_to_all(partial.astype(jnp.bfloat16), "col", 0, 0, tiled=True)
    parts = parts.reshape(devices, rows, partial.shape[1])
    return jnp.sum(parts.astype(jnp.float32), axis=0).astype(jnp.bfloat16)


def product(lhs, rhs, contract):
    return lax.dot_general(lhs, rhs, (contract, ((), ())), preferred_element_type=jnp.float32)


ROWS = ((0,), (0,))
INNER = ((1,), (0,))


def shards(deltas, sketch):
    delta = deltas[0]
    first = lax.all_gather(summed(product(delta, sketch[0], INNER)), "col", axis=0, tiled=True)
    norms = jnp.sum(jnp.square(first.astype(jnp.float32)), axis=0, keepdims=True)
    across = (product(delta, first, ROWS) * lax.rsqrt(norms)).astype(jnp.bfloat16)
    ranged = lax.all_gather(summed(product(delta, across, INNER)), "col", axis=0, tiled=True)
    joined = lax.all_gather(ranged, "task", axis=1, tiled=True)
    inverse = inverse_factor(product(ranged, ranged, ROWS))
    coeffs = dot_exact(inverse, product(ranged, delta, ROWS)).astype(jnp.bfloat16)
    stacked = lax.all_gather(coeffs, "task", axis=0, tiled=True)
    joint = inverse_factor(product(joined, joined, ROWS))
    row_count = joined.shape[0] // lax.axis_size("task")
    joined_rows = lax.dynamic_slice_in_dim(joined, lax.axis_index("task") * row_count, row_count, 0)
    whitened = lax.dot_general(
        joined_rows.astype(jnp.float32),
        joint,
        (((1,), (1,)), ((), ())),
        precision=lax.Precision.HIGHEST,
        preferred_element_type=jnp.float32,
    ).astype(jnp.bfloat16)
    return product(whitened, stacked, INNER).astype(jnp.bfloat16)


def solution(mesh):
    in_specs = (P("task", None, "col"), P("task", "col", None))
    out_specs = P("task", "col")
    return jax.shard_map(shards, mesh=mesh, in_specs=in_specs, out_specs=out_specs, check_vma=False)
```

```python
import jax
import jax.numpy as jnp
from jax import lax
from jax.experimental import pallas as pl
from jax.experimental.pallas import tpu as pltpu
from jax.sharding import PartitionSpec as P

BLOCK = 128
SUB = 8
STRIDE = 4
HALVES = 2
CHUNK = 256


def dot_exact(lhs, rhs):
    return jnp.dot(lhs, rhs, precision=lax.Precision.HIGHEST, preferred_element_type=jnp.float32)


def inverse_factor_block(block):
    groups = BLOCK // SUB
    rows = lax.broadcasted_iota(jnp.int32, (SUB, BLOCK), 0)
    lanes = lax.broadcasted_iota(jnp.int32, (SUB, BLOCK), 1)
    left = [block[g * SUB : (g + 1) * SUB, :] for g in range(groups)]
    right = [(lanes == rows + g * SUB).astype(jnp.float32) for g in range(groups)]
    for start in range(0, BLOCK, STRIDE):
        home, base = divmod(start, SUB)

        def columns_of(g):
            part = left[g]
            return [jnp.broadcast_to(part[:, j : j + 1], (SUB, BLOCK)) for j in range(start, start + STRIDE)]

        columns = columns_of(home)
        pivots = []
        for k in range(STRIDE):
            sub = base + k
            inverse = 1.0 / columns[k][sub : sub + 1, :]
            row_left = left[home][sub : sub + 1, :] * inverse
            row_right = right[home][sub : sub + 1, :] * inverse
            ahead = [columns[m][sub : sub + 1, :] * inverse for m in range(k + 1, STRIDE)]
            pivots.append((row_left, row_right, ahead))
            factor = jnp.where(rows > sub, columns[k], 0.0)
            left[home] = left[home] - factor * row_left
            right[home] = right[home] - factor * row_right
            for m in range(k + 1, STRIDE):
                columns[m] = columns[m] - factor * ahead[m - k - 1]
        for g in range(home + 1, groups):
            columns = columns_of(g)
            for k, (row_left, row_right, ahead) in enumerate(pivots):
                left[g] = left[g] - columns[k] * row_left
                right[g] = right[g] - columns[k] * row_right
                for m in range(k + 1, STRIDE):
                    columns[m] = columns[m] - columns[k] * ahead[m - k - 1]
    scaled = []
    for g in range(groups):
        pivot = jnp.sum(jnp.where(lanes == rows + g * SUB, left[g], 0.0), axis=1, keepdims=True)
        scaled.append(right[g] * lax.rsqrt(pivot))
    return jnp.concatenate(scaled, axis=0)


def eliminate(out_ref, inverse, lo):
    size = out_ref.shape[0]
    hi = lo + BLOCK
    if lo:
        out_ref[lo:hi, :lo] = dot_exact(inverse, out_ref[lo:hi, :lo])
    out_ref[lo:hi, lo:hi] = inverse
    if hi == size:
        return
    panel = dot_exact(inverse, out_ref[lo:hi, hi:])
    out_ref[lo:hi, hi:] = jnp.zeros_like(panel)
    turned = panel.T
    for top in range(hi, size, CHUNK):
        end = min(top + CHUNK, size)
        part = turned[top - hi : end - hi, :]
        out_ref[top:end, top:] -= dot_exact(part, panel[:, top - hi :])
        if lo:
            out_ref[top:end, :lo] -= dot_exact(part, out_ref[lo:hi, :lo])
        out_ref[top:end, lo:hi] = -dot_exact(part, inverse)


def inverse_factor_kernel(gram_ref, out_ref, block_ref):
    steps = gram_ref.shape[0] // BLOCK
    out_ref[...] = gram_ref[...]
    block_ref[...] = gram_ref[:BLOCK, :BLOCK]

    @pl.loop(0, steps)
    def _(step):
        block_ref[...] = inverse_factor_block(block_ref[...])
        for k in range(steps):

            @pl.when(step == k)
            def _():
                eliminate(out_ref, block_ref[...], k * BLOCK)
                if k + 1 < steps:
                    end = (k + 2) * BLOCK
                    block_ref[...] = out_ref[end - BLOCK : end, end - BLOCK : end]


def inverse_factor(gram):
    return pl.pallas_call(
        inverse_factor_kernel,
        out_shape=jax.ShapeDtypeStruct(gram.shape, jnp.float32),
        scratch_shapes=[pltpu.VMEM((BLOCK, BLOCK), jnp.float32)],
        compiler_params=pltpu.CompilerParams(vmem_limit_bytes=48 * 1024 * 1024),
        name="inverse_factor",
    )(gram)


def summed(partial):
    devices = lax.axis_size("col")
    width = partial.shape[1]
    partial = partial.astype(jnp.bfloat16).reshape(devices, HALVES, -1, width)
    halves = []
    total = None
    for half in range(HALVES):
        mine = partial[:, half]
        if half:
            mine, total = lax.optimization_barrier((mine, total))
            halves[-1] = lax.all_gather(total, "col", axis=0)
        parts = lax.all_to_all(mine, "col", 0, 0, tiled=True)
        total = jnp.sum(parts.astype(jnp.float32), axis=0).astype(jnp.bfloat16)
        halves.append(lax.all_gather(total, "col", axis=0))
    return jnp.stack(halves, axis=1).reshape(-1, width)


def product(lhs, rhs, contract):
    return lax.dot_general(lhs, rhs, (contract, ((), ())), preferred_element_type=jnp.float32)


ROWS = ((0,), (0,))
INNER = ((1,), (0,))


def shards(deltas, sketch):
    delta = deltas[0]
    first = summed(product(delta, sketch[0], INNER))
    norms = jnp.sum(jnp.square(first.astype(jnp.float32)), axis=0, keepdims=True)
    across = (product(delta, first, ROWS) * lax.rsqrt(norms)).astype(jnp.bfloat16)
    ranged = summed(product(delta, across, INNER))
    joined = lax.all_gather(ranged, "task", axis=1, tiled=True)
    inverse = inverse_factor(product(ranged, ranged, ROWS))
    coeffs = dot_exact(inverse, product(ranged, delta, ROWS)).astype(jnp.bfloat16)
    stacked = lax.all_gather(coeffs, "task", axis=0, tiled=True)
    joint = inverse_factor(product(joined, joined, ROWS))
    row_count = joined.shape[0] // lax.axis_size("task")
    joined_rows = lax.dynamic_slice_in_dim(joined, lax.axis_index("task") * row_count, row_count, 0)
    whitened = lax.dot_general(
        joined_rows.astype(jnp.float32),
        joint,
        (((1,), (1,)), ((), ())),
        precision=lax.Precision.HIGHEST,
        preferred_element_type=jnp.float32,
    ).astype(jnp.bfloat16)
    return product(whitened, stacked, INNER).astype(jnp.bfloat16)


def solution(mesh):
    in_specs = (P("task", None, "col"), P("task", "col", None))
    out_specs = P("task", "col")
    return jax.shard_map(shards, mesh=mesh, in_specs=in_specs, out_specs=out_specs, check_vma=False)
```
